32 devices in a mesh: tm: 2 (over x), chan: 4 (over y, core), bl: 4 (over z).
Axes of the slice: x: 2, y: 2, z: 4, core: 2. Of those that a mesh axis runs over, the one named last changes fastest.
Arguments:
- voltages: bfloat16 [2, 256, 128, 512], P(None, ('chan', 'bl'), None, 'tm'), may hold values from -6 to 6
Outputs:
- visibilities: bfloat16 [2, 128, 4, 256, 256], P(None, ('chan', 'bl'), 'tm')
The draws below stay inside these ranges and needn't reach their ends.
All inputs are finite; a program needn't handle non-finite values.
Results may differ from the reference program's by a relative error of at most 0.0051.
Values may be sent and summed in bfloat16 or wider, within the bound.
No kernel may reach another device: no remote copies, remote signals or barrier semaphores. Data moves between devices by JAX's collectives and lax.ppermute only.
A program may use at most 64 MiB of HBM per device.

```python
import jax
import jax.numpy as jnp
from jax import lax

SIG = 256
CH_DEV = 8
CHANNELS = 128
HALF = 128
TIME = 512
WIN = 4


def block_levels(stream_key, dims, pieces, least, top_value):
    gain, own = 1.0, jax.random.fold_in(stream_key, 6)
    for position, parts in pieces:
        heights = jnp.exp(jax.random.uniform(jax.random.fold_in(own, position), (parts,), jnp.float32, least / len(pieces), top_value / len(pieces)))
        gain = gain * jnp.repeat(heights, dims[position] // parts).reshape([-1 if axis == position else 1 for axis in range(len(dims))])
    return gain


def scatter_about(key, dims, deviation, limit, shards=(), kind=jnp.bfloat16):
    values = jax.random.normal(key, dims, jnp.float32) * deviation
    if len(shards) > 0:
        values = block_levels(key, dims, shards, -0.22, 0.18) * values
    return jnp.clip(values, min=-limit, max=limit).astype(kind)


def setup_inputs(seed: int = 0) -> dict:
    key_list = jax.random.split(jax.random.key(seed), 2)
    voltages = scatter_about(key_list[0], (2, SIG, CHANNELS, TIME), 1.0, 6.0, ((1, 16), (3, 2)))
    return dict(voltages=voltages)


def tapers(length):
    steps = jnp.arange(length, dtype=jnp.float32)
    taper_early = jnp.sin(jnp.pi * (steps + 0.5) / (2.0 * length))
    taper_late = jnp.sin(jnp.pi * (steps + 0.5 + length) / (2.0 * length))
    return taper_early, taper_late


def weighted(block, taper):
    return (block.astype(jnp.float32) * taper).astype(jnp.bfloat16)


def products(stacked):
    signals = stacked.shape[0] // 2
    wide = stacked.astype(jnp.float32)
    gram = jnp.einsum("pct,qct->cpq", wide, wide, precision=lax.Precision.HIGHEST)
    real_part = gram[:, :signals, :signals] + gram[:, signals:, signals:]
    imag_part = gram[:, signals:, :signals] - gram[:, :signals, signals:]
    return real_part, imag_part


def reference(voltages):
    taper_early, taper_late = tapers(HALF)
    groups = CHANNELS // CH_DEV
    halves = TIME // HALF
    scale = 1.0 / HALF

    def one_group(group):
        block = lax.dynamic_slice_in_dim(voltages, group * CH_DEV, CH_DEV, 2)
        stacked = block.reshape(2 * SIG, CH_DEV, TIME)
        previous = (jnp.zeros((CH_DEV, SIG, SIG), jnp.float32), jnp.zeros((CH_DEV, SIG, SIG), jnp.float32))
        real_list = []
        imag_list = []
        for index in range(halves):
            piece = stacked[:, :, index * HALF:(index + 1) * HALF]
            late_real, late_imag = products(weighted(piece, taper_late))
            real_list.append(((late_real + previous[0]) * scale).astype(jnp.bfloat16))
            imag_list.append(((late_imag + previous[1]) * scale).astype(jnp.bfloat16))
            previous = products(weighted(piece, taper_early))
        return jnp.stack([jnp.stack(real_list, 1), jnp.stack(imag_list, 1)], 0)

    result = lax.map(one_group, jnp.arange(groups, dtype=jnp.int32))
    return jnp.transpose(result, (1, 0, 2, 3, 4, 5)).reshape(2, CHANNELS, WIN, SIG, SIG)
```

```python
import functools

import jax
import jax.numpy as jnp
from jax import lax
from jax.experimental import pallas as pl
from jax.experimental.pallas import tpu as pltpu
from jax.sharding import PartitionSpec as P

HALF = 128
ROWS = 16


def passed_along(block, axis, distance):
    devices = range(lax.axis_size(axis))
    route = [(i - distance, i) for i in devices if i - distance in devices]
    return lax.ppermute(block, axis, route)


def tapers(length):
    steps = jnp.arange(length, dtype=jnp.float32)
    taper_early = jnp.sin(jnp.pi * (steps + 0.5) / (2.0 * length))
    taper_late = jnp.sin(jnp.pi * (steps + 0.5 + length) / (2.0 * length))
    return jnp.stack([taper_early, taper_late])


def turned(piece):
    parts, signals, channels, samples = piece.shape
    devices = lax.axis_size("chan") * lax.axis_size("bl")
    by_channel = jnp.transpose(piece, (2, 0, 1, 3))
    swapped = lax.all_to_all(by_channel, ("chan", "bl"), split_axis=0, concat_axis=0, tiled=True)
    swapped = swapped.reshape(devices, channels // devices, parts, signals, samples)
    if signals % ROWS:
        swapped = jnp.transpose(swapped, (1, 2, 0, 3, 4))
        swapped = swapped.reshape(1, channels // devices, parts, devices * signals, samples)
    return swapped


def correlate(taper_ref, *refs):
    blocks, out_ref = refs[:-1], refs[-1]
    taper_early, taper_late = taper_ref[0:1, :], taper_ref[1:2, :]
    scale = 1.0 / HALF

    def part(block, index, taper):
        values = block[:, 0, index]
        values = values.reshape(values.shape[0] * values.shape[1], values.shape[2])
        return (values.astype(jnp.float32) * taper).astype(jnp.bfloat16)

    for window in range(len(blocks) - 1):
        late_a, late_b = (part(blocks[window + 1], i, taper_late) for i in range(2))
        early_a, early_b = (part(blocks[window], i, taper_early) for i in range(2))
        straight = jnp.concatenate([late_a, late_b, early_a, early_b], axis=1)
        crossed = jnp.concatenate([late_b, -late_a, early_b, -early_a], axis=1)
        for index, left in enumerate((straight, crossed)):
            gram = lax.dot_general(left, straight, (((1,), (1,)), ((), ())), preferred_element_type=jnp.float32)
            out_ref[index, 0, window] = (gram * scale).astype(jnp.bfloat16)


def correlated(blocks):
    sources, channels, parts, signals, samples = blocks[0].shape
    windows = len(blocks) - 1
    everyone = sources * signals
    spec = pl.BlockSpec((sources, 1, parts, signals, samples), lambda c: (0, c, 0, 0, 0))
    flops = channels * windows * 2 * parts * everyone * everyone * 2 * parts * samples
    return pl.pallas_call(
        correlate,
        grid=(channels,),
        in_specs=[pl.BlockSpec((2, samples), lambda c: (0, 0))] + [spec] * len(blocks),
        out_specs=pl.BlockSpec((parts, 1, windows, everyone, everyone), lambda c: (0, c, 0, 0, 0)),
        out_shape=jax.ShapeDtypeStruct((parts, channels, windows, everyone, everyone), jnp.bfloat16),
        cost_estimate=pl.CostEstimate(flops=flops, bytes_accessed=8 << 20, transcendentals=0),
        name="correlate",
    )(tapers(samples), *blocks)


def local(voltages):
    halves = voltages.shape[3] // HALF
    pieces = [voltages[:, :, :, i * HALF : (i + 1) * HALF] for i in range(halves)]
    last = turned(pieces[-1])
    received = passed_along(last, "tm", 1)
    blocks = [received]
    for piece in pieces[:-1]:
        piece, last = lax.optimization_barrier((piece, last))
        blocks.append(turned(piece))
    return correlated(blocks + [last])


def solution(mesh):
    return jax.shard_map(
        local,
        mesh=mesh,
        in_specs=(P(None, ("chan", "bl"), None, "tm"),),
        out_specs=P(None, ("chan", "bl"), "tm", None, None),
        check_vma=False,
    )
```

```python
import jax
import jax.numpy as jnp
import numpy as np
from jax import lax
from jax.experimental import pallas as pl
from jax.experimental.pallas import tpu as pltpu
from jax.sharding import PartitionSpec as P


HALF = 128
ROWS = 16


def passed_along(block, axis, distance):
    devices = range(lax.axis_size(axis))
    route = [(i - distance, i) for i in devices if i - distance in devices]
    return lax.ppermute(block, axis, route)


def exchanged(block, axis, mask):
    return lax.ppermute(block, axis, [(i, i ^ mask) for i in range(lax.axis_size(axis))])


def tapers(length):
    steps = jnp.arange(length, dtype=jnp.float32)
    taper_early = jnp.sin(jnp.pi * (steps + 0.5) / (2.0 * length))
    taper_late = jnp.sin(jnp.pi * (steps + 0.5 + length) / (2.0 * length))
    return jnp.stack([taper_early, taper_late])


def correlate(rows_ref, taper_ref, *refs, halves, pieces):
    blocks = [refs[h * pieces : (h + 1) * pieces] for h in range(halves)]
    out_ref, stack_ref = refs[-2], refs[-1]
    channel = pl.program_id(0)
    scale = 1.0 / HALF

    def place(window, half, which):
        taper = taper_ref[which : which + 1, :]
        slot = 0
        for block in blocks[half]:
            for first in range(block.shape[0]):
                for second in range(block.shape[1]):
                    row = rows_ref[slot]
                    slot += 1
                    height = block.shape[4]
                    row = pl.multiple_of(row, height)
                    for part in range(2):
                        values = block[first, second, channel, part].astype(jnp.float32)
                        column = (2 * (1 - which) + part) * HALF
                        stack_ref[window, pl.ds(row, height), column : column + HALF] = (values * taper).astype(jnp.bfloat16)

    for window in range(halves - 1):
        place(window, window + 1, 1)
        place(window, window, 0)
    for window in range(halves - 1):
        straight = stack_ref[window]
        late_a, late_b, early_a, early_b = (straight[:, i * HALF : (i + 1) * HALF] for i in range(4))
        crossed = jnp.concatenate([late_b, -late_a, early_b, -early_a], axis=1)
        for index, left in enumerate((straight, crossed)):
            gram = lax.dot_general(left, straight, (((1,), (1,)), ((), ())), preferred_element_type=jnp.float32)
            out_ref[index, 0, window] = (gram * scale).astype(jnp.bfloat16)


def correlated(rows, blocks):
    halves, pieces = len(blocks), len(blocks[0])
    channels, parts, height, samples = blocks[0][0].shape[2:]
    windows, everyone = halves - 1, rows.shape[0] * height
    flops = channels * windows * 2 * parts * everyone * everyone * 2 * parts * samples

    def body(*refs):
        correlate(*refs, halves=halves, pieces=pieces)

    flat = [array for half in blocks for array in half]
    return pl.pallas_call(
        body,
        grid=(channels,),
        in_specs=[pl.BlockSpec(memory_space=pltpu.SMEM), pl.BlockSpec(memory_space=pltpu.VMEM)]
        + [pl.BlockSpec(memory_space=pltpu.VMEM)] * len(flat),
        out_specs=pl.BlockSpec((parts, 1, windows, everyone, everyone), lambda c: (0, c, 0, 0, 0)),
        out_shape=jax.ShapeDtypeStruct((parts, channels, windows, everyone, everyone), jnp.bfloat16),
        scratch_shapes=[pltpu.VMEM((windows, everyone, 2 * parts * samples), jnp.bfloat16)],
        cost_estimate=pl.CostEstimate(flops=flops, bytes_accessed=8 << 20, transcendentals=0),
        compiler_params=pltpu.CompilerParams(vmem_limit_bytes=12 << 20),
        name="correlate",
    )(rows, tapers(samples), *flat)


def at(array, index):
    zero = jnp.uint32(0)
    start = [index] + [zero] * (array.ndim - 1)
    return lax.dynamic_slice(array, start, (1,) + array.shape[1:])[0]


def staged(voltages):
    parts, signals, channels, samples = voltages.shape
    chans, bls = lax.axis_size("chan"), lax.axis_size("bl")
    each = channels // (chans * bls)
    halves = samples // HALF
    chan, bl = (lax.axis_index(axis).astype(jnp.uint32) for axis in ("chan", "bl"))
    masks, shifts = range(chans), range(bls)
    order = shifts[1:]
    split = voltages.reshape(parts, signals, chans, bls, each, samples)
    peer = [chan ^ np.uint32(m) for m in masks]
    ahead = [bl ^ np.uint32(s) for s in shifts]
    rows = jnp.stack([(peer[m] * np.uint32(bls) + ahead[s]) * np.uint32(signals) for s in shifts for m in masks])
    rows = rows.astype(jnp.int32)
    voltages, peer, ahead, rows = lax.optimization_barrier((voltages, peer, ahead, rows))

    def cut(half):
        piece = split[..., half * HALF : (half + 1) * HALF]
        return piece

    def over_chan_first(half):
        piece = jnp.transpose(cut(half), (2, 3, 4, 0, 1, 5))
        held = [at(piece, peer[0])]
        for mask in masks[1:]:
            held.append(exchanged(at(piece, peer[mask]), "chan", mask))
        own = jnp.stack([at(array, ahead[0]) for array in held])
        result = {0: own}
        for shift in order:
            outgoing = jnp.stack([at(array, ahead[shift]) for array in held])
            result[shift] = exchanged(outgoing, "bl", shift)
        return [result[s][None] for s in shifts]

    def over_bl_first(half):
        piece = jnp.transpose(cut(half), (3, 2, 4, 0, 1, 5))
        held = {0: at(piece, ahead[0])}
        for shift in order:
            held[shift] = exchanged(at(piece, ahead[shift]), "bl", shift)
        groups = [list(shifts[: bls // 2]), list(shifts[bls // 2 :])]
        here, along = {}, {}
        for group in groups:
            turned = [jnp.stack([at(held[s], peer[0]) for s in group])]
            for mask in masks[1:]:
                outgoing = jnp.stack([at(held[s], peer[mask]) for s in group])
                turned.append(exchanged(outgoing, "chan", mask))
            whole = jnp.stack(turned, 1)
            passed = passed_along(whole, "tm", 1)
            for i, s in enumerate(group):
                here[s], along[s] = whole[i : i + 1], passed[i : i + 1]
        return [here[s] for s in shifts], [along[s] for s in shifts]

    last, received = over_bl_first(halves - 1)
    blocks = [received] + [over_chan_first(h) for h in range(halves - 1)] + [last]
    return correlated(rows, blocks)


def turned(piece):
    parts, signals, channels, samples = piece.shape
    devices = lax.axis_size("chan") * lax.axis_size("bl")
    by_channel = jnp.transpose(piece, (2, 0, 1, 3))
    swapped = lax.all_to_all(by_channel, ("chan", "bl"), split_axis=0, concat_axis=0, tiled=True)
    swapped = swapped.reshape(devices, channels // devices, parts, signals, samples)
    swapped = jnp.transpose(swapped, (1, 2, 0, 3, 4))
    return swapped.reshape(1, 1, channels // devices, parts, devices * signals, samples)


def direct(voltages):
    halves = voltages.shape[3] // HALF
    pieces = [voltages[:, :, :, i * HALF : (i + 1) * HALF] for i in range(halves)]
    last = turned(pieces[-1])
    received = passed_along(last, "tm", 1)
    blocks = [[received]] + [[turned(piece)] for piece in pieces[:-1]] + [[last]]
    return correlated(jnp.zeros((1,), jnp.int32), blocks)


def placed(voltages):
    chans, bls = lax.axis_size("chan"), lax.axis_size("bl")
    if voltages.shape[1] % ROWS == 0 and chans <= 4 and not (chans & (chans - 1) or bls & (bls - 1)):
        return staged(voltages)
    return direct(voltages)


def solution(mesh):
    return jax.shard_map(
        placed,
        mesh=mesh,
        in_specs=(P(None, ("chan", "bl"), None, "tm"),),
        out_specs=P(None, ("chan", "bl"), "tm", None, None),
        check_vma=False,
    )
```

```python
import jax
import jax.numpy as jnp
from jax import lax
from jax.experimental import pallas as pl
from jax.experimental.pallas import tpu as pltpu
from jax.sharding import PartitionSpec as P


HALF = 128
ROWS = 16


def passed_along(block, axis, distance):
    devices = range(lax.axis_size(axis))
    route = [(i - distance, i) for i in devices if i - distance in devices]
    return lax.ppermute(block, axis, route)


def exchanged(block, axis, mask):
    return lax.ppermute(block, axis, [(i, i ^ mask) for i in range(lax.axis_size(axis))])


def tapers(length):
    steps = jnp.arange(length, dtype=jnp.float32)
    taper_early = jnp.sin(jnp.pi * (steps + 0.5) / (2.0 * length))
    taper_late = jnp.sin(jnp.pi * (steps + 0.5 + length) / (2.0 * length))
    return jnp.stack([taper_early, taper_late])


def correlate(taper_ref, *refs, halves, pieces, channels, paired):
    blocks = [refs[h * pieces : (h + 1) * pieces] for h in range(halves)]
    out_ref, even_ref, odd_ref = refs[-3:]
    step = pl.program_id(0)
    scale = 1.0 / HALF
    if paired:
        chan, bl, bls = lax.axis_index("chan"), lax.axis_index("bl"), lax.axis_size("bl")

    def place(stack_ref, channel, window, half, which):
        taper = taper_ref[which : which + 1, :]
        for shift, block in enumerate(blocks[half]):
            height = block.shape[4]
            for first in range(block.shape[0]):
                for second in range(block.shape[1]):
                    row = 0
                    if paired:
                        row = pl.multiple_of(((chan ^ second) * bls + (bl ^ shift)) * height, height)
                    for part in range(2):
                        values = block[first, second, channel, part].astype(jnp.float32)
                        column = (2 * (1 - which) + part) * HALF
                        stack_ref[window, pl.ds(row, height), column : column + HALF] = (values * taper).astype(jnp.bfloat16)

    def fill(stack_ref, channel, window):
        place(stack_ref, channel, window, window + 1, 1)
        place(stack_ref, channel, window, window, 0)

    def store(index, window, gram):
        out_ref[index, 0, window] = (gram * scale).astype(jnp.bfloat16)

    def both(now_ref, next_ref):
        following = jnp.minimum(step + 1, channels - 1)
        waiting = None
        for window in range(halves - 1):
            straight = now_ref[window]
            late_a, late_b, early_a, early_b = (straight[:, i * HALF : (i + 1) * HALF] for i in range(4))
            crossed = jnp.concatenate([late_b, -late_a, early_b, -early_a], axis=1)
            for index, left in enumerate((straight, crossed)):
                gram = lax.dot_general(left, straight, (((1,), (1,)), ((), ())), preferred_element_type=jnp.float32)
                if waiting is not None:
                    store(*waiting)
                half, which = (window + 1, 1) if index == 0 else (window, 0)
                place(next_ref, following, window, half, which)
                waiting = (index, window, gram)
        store(*waiting)

    @pl.when(step == 0)
    def _():
        for window in range(halves - 1):
            fill(even_ref, step, window)

    @pl.when(step % 2 == 0)
    def _():
        both(even_ref, odd_ref)

    @pl.when(step % 2 == 1)
    def _():
        both(odd_ref, even_ref)


def correlated(blocks, paired):
    halves, pieces = len(blocks), len(blocks[0])
    channels, parts, height, samples = blocks[0][0].shape[2:]
    windows = halves - 1
    everyone = sum(array.shape[1] for array in blocks[0]) * height
    flops = channels * windows * 2 * parts * everyone * everyone * 2 * parts * samples

    def body(*refs):
        correlate(*refs, halves=halves, pieces=pieces, channels=channels, paired=paired)

    flat = [array for half in blocks for array in half]
    return pl.pallas_call(
        body,
        grid=(channels,),
        in_specs=[pl.BlockSpec(memory_space=pltpu.VMEM)]
        + [pl.BlockSpec(memory_space=pltpu.VMEM)] * len(flat),
        out_specs=pl.BlockSpec((parts, 1, windows, everyone, everyone), lambda c: (0, c, 0, 0, 0)),
        out_shape=jax.ShapeDtypeStruct((parts, channels, windows, everyone, everyone), jnp.bfloat16),
        scratch_shapes=[pltpu.VMEM((windows, everyone, 2 * parts * samples), jnp.bfloat16)] * 2,
        cost_estimate=pl.CostEstimate(flops=flops, bytes_accessed=8 << 20, transcendentals=0),
        compiler_params=pltpu.CompilerParams(vmem_limit_bytes=12 << 20),
        name="correlate",
    )(tapers(samples), *flat)


def picked(held, axis):
    size, block = held[0].shape[0], held[0].shape[1:]

    def body(*refs):
        mine = lax.axis_index(axis)
        for mask in range(size):
            for place in range(len(held)):
                refs[len(held) + mask][place] = refs[place][mine ^ mask]

    return pl.pallas_call(
        body,
        in_specs=[pl.BlockSpec(memory_space=pltpu.VMEM)] * len(held),
        out_specs=[pl.BlockSpec(memory_space=pltpu.VMEM)] * size,
        out_shape=[jax.ShapeDtypeStruct((len(held),) + block, held[0].dtype)] * size,
        compiler_params=pltpu.CompilerParams(vmem_limit_bytes=4 << 20),
        cost_estimate=pl.CostEstimate(flops=0, bytes_accessed=1 << 20, transcendentals=0),
    )(*held)


def staged(voltages):
    parts, signals, channels, samples = voltages.shape
    chans, bls = lax.axis_size("chan"), lax.axis_size("bl")
    each = channels // (chans * bls)
    halves = samples // HALF
    masks, shifts = range(chans), range(bls)
    order = shifts[1:]
    split = voltages.reshape(parts, signals, chans, bls, each, samples)

    def cut(half):
        def body(whole_ref, *rest):
            outs, sems = rest[:-1], rest[-1]
            axis, count = ("bl", bls) if half == halves - 1 else ("chan", chans)
            mine, copies = lax.axis_index(axis), []
            for mask in range(count):
                place = (slice(None), slice(None), pl.ds(mine ^ mask, 1))
                if axis == "bl":
                    place = (slice(None), slice(None), slice(None), pl.ds(mine ^ mask, 1))
                source = whole_ref.at[place + (Ellipsis, pl.ds(half * HALF, HALF))]
                copies.append(pltpu.make_async_copy(source, outs[mask], sems.at[mask]))
            for copy in copies:
                copy.start()
            for copy in copies:
                copy.wait()

        bl_part = half == halves - 1
        shape = (parts, signals, chans if bl_part else 1, 1 if bl_part else bls, each, HALF)
        count = bls if bl_part else chans
        return pl.pallas_call(
            body,
            in_specs=[pl.BlockSpec(memory_space=pl.ANY)],
            out_specs=[pl.BlockSpec(memory_space=pltpu.VMEM)] * count,
            out_shape=[jax.ShapeDtypeStruct(shape, voltages.dtype)] * count,
            scratch_shapes=[pltpu.SemaphoreType.DMA((count,))],
            compiler_params=pltpu.CompilerParams(vmem_limit_bytes=4 << 20),
            cost_estimate=pl.CostEstimate(flops=0, bytes_accessed=2 << 20, transcendentals=0),
        )(split)

    def sliced(pieces, mask):
        part = pieces[mask].reshape(parts, signals, -1, each, HALF)
        return jnp.transpose(part, (2, 3, 0, 1, 4))

    def over_chan_first(half):
        piece = cut(half)
        held = [sliced(piece, 0)]
        for mask in masks[1:]:
            held.append(exchanged(sliced(piece, mask), "chan", mask))
        outgoing = picked(held, "bl")
        result = {0: outgoing[0]}
        for shift in order:
            result[shift] = exchanged(outgoing[shift], "bl", shift)
        return [result[s][None] for s in shifts]

    def over_bl_first(half):
        piece = cut(half)
        held = {0: sliced(piece, 0)}
        for shift in order:
            held[shift] = exchanged(sliced(piece, shift), "bl", shift)
        groups = [list(shifts[: bls // 2]), list(shifts[bls // 2 :])]
        here, along = {}, {}
        for group in groups:
            outgoing = picked([held[s] for s in group], "chan")
            turned = [outgoing[0]]
            for mask in masks[1:]:
                turned.append(exchanged(outgoing[mask], "chan", mask))
            whole = jnp.stack(turned, 1)
            passed = passed_along(whole, "tm", 1)
            for i, s in enumerate(group):
                here[s], along[s] = whole[i : i + 1], passed[i : i + 1]
        return [here[s] for s in shifts], [along[s] for s in shifts]

    last, received = over_bl_first(halves - 1)
    blocks = [received] + [over_chan_first(h) for h in range(halves - 1)] + [last]
    return correlated(blocks, True)


def turned(piece):
    parts, signals, channels, samples = piece.shape
    devices = lax.axis_size("chan") * lax.axis_size("bl")
    by_channel = jnp.transpose(piece, (2, 0, 1, 3))
    swapped = lax.all_to_all(by_channel, ("chan", "bl"), split_axis=0, concat_axis=0, tiled=True)
    swapped = swapped.reshape(devices, channels // devices, parts, signals, samples)
    swapped = jnp.transpose(swapped, (1, 2, 0, 3, 4))
    return swapped.reshape(1, 1, channels // devices, parts, devices * signals, samples)


def direct(voltages):
    halves = voltages.shape[3] // HALF
    pieces = [voltages[:, :, :, i * HALF : (i + 1) * HALF] for i in range(halves)]
    last = turned(pieces[-1])
    received = passed_along(last, "tm", 1)
    blocks = [[received]] + [[turned(piece)] for piece in pieces[:-1]] + [[last]]
    return correlated(blocks, False)


def placed(voltages):
    chans, bls = lax.axis_size("chan"), lax.axis_size("bl")
    if voltages.shape[1] % ROWS == 0 and chans <= 4 and not (chans & (chans - 1) or bls & (bls - 1)):
        return staged(voltages)
    return direct(voltages)


def solution(mesh):
    return jax.shard_map(
        placed,
        mesh=mesh,
        in_specs=(P(None, ("chan", "bl"), None, "tm"),),
        out_specs=P(None, ("chan", "bl"), "tm", None, None),
        check_vma=False,
    )
```

```python
import jax
import jax.numpy as jnp
from jax import lax
from jax.experimental import pallas as pl
from jax.experimental.pallas import tpu as pltpu
from jax.sharding import PartitionSpec as P


HALF = 128
ROWS = 16


def passed_along(block, axis, distance):
    devices = range(lax.axis_size(axis))
    route = [(i - distance, i) for i in devices if i - distance in devices]
    return lax.ppermute(block, axis, route)


def exchanged(block, axis, mask):
    return lax.ppermute(block, axis, [(i, i ^ mask) for i in range(lax.axis_size(axis))])


def tapers(length):
    steps = jnp.arange(length, dtype=jnp.float32)
    taper_early = jnp.sin(jnp.pi * (steps + 0.5) / (2.0 * length))
    taper_late = jnp.sin(jnp.pi * (steps + 0.5 + length) / (2.0 * length))
    return jnp.stack([taper_early, taper_late])


def correlate(taper_ref, *refs, layout, channels, paired):
    halves = len(layout)
    out_ref, even_ref, odd_ref = refs[-3:]
    step = pl.program_id(0)
    scale = 1.0 / HALF
    if paired:
        chan, bl, bls = lax.axis_index("chan"), lax.axis_index("bl"), lax.axis_size("bl")

    def place(stack_ref, channel, window, half, which):
        taper = taper_ref[which : which + 1, :]
        for slot, shifts, masks, offset in layout[half]:
            block = refs[slot]
            height = block.shape[4]
            for first, shift in enumerate(shifts):
                for second, mask in enumerate(masks):
                    row = 0
                    if paired:
                        row = pl.multiple_of(((chan ^ mask) * bls + (bl ^ shift)) * height, height)
                    for part in range(2):
                        values = block[first, second, channel + offset, part].astype(jnp.float32)
                        column = (2 * (1 - which) + part) * HALF
                        stack_ref[window, pl.ds(row, height), column : column + HALF] = (values * taper).astype(jnp.bfloat16)

    def store(index, window, gram):
        out_ref[index, 0, window] = (gram * scale).astype(jnp.bfloat16)

    def both(now_ref, next_ref):
        following = jnp.minimum(step + 1, channels - 1)
        waiting = None
        for window in range(halves - 1):
            straight = now_ref[window]
            late_a, late_b, early_a, early_b = (straight[:, i * HALF : (i + 1) * HALF] for i in range(4))
            crossed = jnp.concatenate([late_b, -late_a, early_b, -early_a], axis=1)
            for index, left in enumerate((straight, crossed)):
                gram = lax.dot_general(left, straight, (((1,), (1,)), ((), ())), preferred_element_type=jnp.float32)
                if waiting is not None:
                    store(*waiting)
                half, which = (window + 1, 1) if index == 0 else (window, 0)
                place(next_ref, following, window, half, which)
                waiting = (index, window, gram)
        store(*waiting)

    @pl.when(step == 0)
    def _():
        for window in range(halves - 1):
            place(even_ref, step, window, window + 1, 1)
            place(even_ref, step, window, window, 0)

    @pl.when(step % 2 == 0)
    def _():
        both(even_ref, odd_ref)

    @pl.when(step % 2 == 1)
    def _():
        both(odd_ref, even_ref)


def correlated(blocks, total, base, paired, before):
    channels = min(array.shape[2] for half in blocks for array, _, _ in half)
    parts, height, samples = blocks[0][0][0].shape[3:]
    windows = len(blocks) - 1
    everyone = sum(len(shifts) * len(masks) for _, shifts, masks in blocks[0]) * height
    flops = channels * windows * 2 * parts * everyone * everyone * 2 * parts * samples
    layout, flat = [], []
    for half in blocks:
        layout.append([])
        for array, shifts, masks in half:
            layout[-1].append((len(flat), shifts, masks, base if array.shape[2] > channels else 0))
            flat.append(array)
    given = [] if before is None else [before]

    def body(taper_ref, *refs):
        correlate(taper_ref, *refs[len(given) :], layout=layout, channels=channels, paired=paired)

    return pl.pallas_call(
        body,
        grid=(channels,),
        in_specs=[pl.BlockSpec(memory_space=pltpu.VMEM)]
        + [pl.BlockSpec(memory_space=pl.ANY)] * len(given)
        + [pl.BlockSpec(memory_space=pltpu.VMEM)] * len(flat),
        out_specs=pl.BlockSpec((parts, 1, windows, everyone, everyone), lambda c: (0, c + base, 0, 0, 0)),
        out_shape=jax.ShapeDtypeStruct((parts, total, windows, everyone, everyone), jnp.bfloat16),
        input_output_aliases={1: 0} if given else {},
        scratch_shapes=[pltpu.VMEM((windows, everyone, 2 * parts * samples), jnp.bfloat16)] * 2,
        cost_estimate=pl.CostEstimate(flops=flops, bytes_accessed=4 << 20, transcendentals=0),
        compiler_params=pltpu.CompilerParams(vmem_limit_bytes=12 << 20),
    )(tapers(samples), *given, *flat)


def picked(held, axis, cuts):
    size, block, kind = held[0].shape[0], held[0].shape[1:], held[0].dtype

    def body(*refs):
        mine, outs = lax.axis_index(axis), iter(refs[len(held) :])
        for mask in range(size):
            for start, stop in cuts[mask]:
                out_ref = next(outs)
                for place in range(len(held)):
                    out_ref[place] = refs[place][mine ^ mask, start:stop]

    shapes = [(len(held), stop - start) + block[1:] for mask in range(size) for start, stop in cuts[mask]]
    outs = pl.pallas_call(
        body,
        in_specs=[pl.BlockSpec(memory_space=pltpu.VMEM)] * len(held),
        out_specs=[pl.BlockSpec(memory_space=pltpu.VMEM)] * len(shapes),
        out_shape=[jax.ShapeDtypeStruct(shape, kind) for shape in shapes],
        compiler_params=pltpu.CompilerParams(vmem_limit_bytes=4 << 20),
        cost_estimate=pl.CostEstimate(flops=0, bytes_accessed=1 << 20, transcendentals=0),
    )(*held)
    outs = iter(outs)
    return [[next(outs) for _ in cuts[mask]] for mask in range(size)]


def staged(voltages):
    parts, signals, channels, samples = voltages.shape
    chans, bls = lax.axis_size("chan"), lax.axis_size("bl")
    each = channels // (chans * bls)
    halves = samples // HALF
    masks, shifts = range(chans), range(bls)
    order = shifts[1:]
    split = voltages.reshape(parts, signals, chans, bls, each, samples)

    def cut(half):
        def body(whole_ref, *rest):
            outs, sems = rest[:-1], rest[-1]
            axis, count = ("bl", bls) if half == halves - 1 else ("chan", chans)
            mine, copies = lax.axis_index(axis), []
            for mask in range(count):
                place = (slice(None), slice(None), pl.ds(mine ^ mask, 1))
                if axis == "bl":
                    place = (slice(None), slice(None), slice(None), pl.ds(mine ^ mask, 1))
                source = whole_ref.at[place + (Ellipsis, pl.ds(half * HALF, HALF))]
                copies.append(pltpu.make_async_copy(source, outs[mask], sems.at[mask]))
            for copy in copies:
                copy.start()
            for copy in copies:
                copy.wait()

        bl_part = half == halves - 1
        shape = (parts, signals, chans if bl_part else 1, 1 if bl_part else bls, each, HALF)
        count = bls if bl_part else chans
        return pl.pallas_call(
            body,
            in_specs=[pl.BlockSpec(memory_space=pl.ANY)],
            out_specs=[pl.BlockSpec(memory_space=pltpu.VMEM)] * count,
            out_shape=[jax.ShapeDtypeStruct(shape, voltages.dtype)] * count,
            scratch_shapes=[pltpu.SemaphoreType.DMA((count,))],
            compiler_params=pltpu.CompilerParams(vmem_limit_bytes=4 << 20),
            cost_estimate=pl.CostEstimate(flops=0, bytes_accessed=2 << 20, transcendentals=0),
        )(split)

    def sliced(pieces, mask):
        part = pieces[mask].reshape(parts, signals, -1, each, HALF)
        return jnp.transpose(part, (2, 3, 0, 1, 4))

    whole = [(0, each)]
    middle = each // 2 if each % 2 == 0 else each
    split_cuts = [(0, middle), (middle, each)] if middle < each else whole

    def over_chan_first(half):
        pieces = cut(half)
        held = [sliced(pieces, 0)]
        for mask in masks[1:]:
            held.append(exchanged(sliced(pieces, mask), "chan", mask))
        outgoing = picked(held, "bl", [whole] + [split_cuts] * (bls - 1))
        result = [[(outgoing[0][0][None], [0], masks)] for _ in split_cuts]
        for part in range(len(split_cuts)):
            for shift in order:
                moved = exchanged(outgoing[shift][part], "bl", shift)
                result[part].append((moved[None], [shift], masks))
        return result

    def over_bl_first(half):
        pieces = cut(half)
        held = {0: sliced(pieces, 0)}
        for shift in order:
            held[shift] = exchanged(sliced(pieces, shift), "bl", shift)
        groups = [list(shifts[: bls // 2]), list(shifts[bls // 2 :])] if bls > 1 else [[0]]
        here, along = [], [[] for _ in split_cuts]
        for group in groups:
            outgoing = picked([held[s] for s in group], "chan", [whole] * chans)
            turned = [outgoing[0][0]]
            for mask in masks[1:]:
                turned.append(exchanged(outgoing[mask][0], "chan", mask))
            here += [(turned[mask][:, None], group, [mask]) for mask in masks]
            cuts = split_cuts if group is groups[-1] else whole
            for part, (start, stop) in enumerate(cuts):
                stacked = jnp.stack([array[:, start:stop] for array in turned], 1)
                passed = passed_along(stacked, "tm", 1)
                for target in along if len(cuts) == 1 else along[part : part + 1]:
                    target.append((passed, group, masks))
        return here, along

    last, received = over_bl_first(halves - 1)
    others = [over_chan_first(h) for h in range(halves - 1)]
    result = None
    for part, (start, stop) in enumerate(split_cuts):
        blocks = [received[part]] + [other[part] for other in others] + [last]
        result = correlated(blocks, each, start, True, result)
    return result


def turned(piece):
    parts, signals, channels, samples = piece.shape
    devices = lax.axis_size("chan") * lax.axis_size("bl")
    by_channel = jnp.transpose(piece, (2, 0, 1, 3))
    swapped = lax.all_to_all(by_channel, ("chan", "bl"), split_axis=0, concat_axis=0, tiled=True)
    swapped = swapped.reshape(devices, channels // devices, parts, signals, samples)
    swapped = jnp.transpose(swapped, (1, 2, 0, 3, 4))
    return swapped.reshape(1, 1, channels // devices, parts, devices * signals, samples)


def direct(voltages):
    halves = voltages.shape[3] // HALF
    pieces = [voltages[:, :, :, i * HALF : (i + 1) * HALF] for i in range(halves)]
    last = turned(pieces[-1])
    received = passed_along(last, "tm", 1)
    blocks = [received] + [turned(piece) for piece in pieces[:-1]] + [last]
    return correlated([[(block, [0], [0])] for block in blocks], last.shape[2], 0, False, None)


def placed(voltages):
    chans, bls = lax.axis_size("chan"), lax.axis_size("bl")
    if voltages.shape[1] % ROWS == 0 and chans <= 4 and not (chans & (chans - 1) or bls & (bls - 1)):
        return staged(voltages)
    return direct(voltages)


def solution(mesh):
    return jax.shard_map(
        placed,
        mesh=mesh,
        in_specs=(P(None, ("chan", "bl"), None, "tm"),),
        out_specs=P(None, ("chan", "bl"), "tm", None, None),
        check_vma=False,
    )
```

```python
import jax
import jax.numpy as jnp
from jax import lax
from jax.experimental import pallas as pl
from jax.experimental.pallas import tpu as pltpu
from jax.sharding import PartitionSpec as P


HALF = 128
ROWS = 16


def passed_along(block, axis, distance):
    size = lax.axis_size(axis)
    return lax.ppermute(block, axis, [(i, (i + distance) % size) for i in range(size)])


def exchanged(block, axis, mask):
    return lax.ppermute(block, axis, [(i, i ^ mask) for i in range(lax.axis_size(axis))])


def tapers(length):
    steps = jnp.arange(length, dtype=jnp.float32)
    taper_early = jnp.sin(jnp.pi * (steps + 0.5) / (2.0 * length))
    taper_late = jnp.sin(jnp.pi * (steps + 0.5 + length) / (2.0 * length))
    return jnp.stack([taper_early, taper_late])


def correlate(taper_ref, *refs, layout, channels, paired):
    halves = len(layout)
    out_ref, even_ref, odd_ref = refs[-3:]
    step = pl.program_id(0)
    scale = 1.0 / HALF
    if paired:
        chan, bl, bls = lax.axis_index("chan"), lax.axis_index("bl"), lax.axis_size("bl")

    def place(stack_ref, channel, window, half, which):
        taper = taper_ref[which : which + 1, :]
        if half == 0:
            taper = jnp.where(lax.axis_index("tm") > 0, taper, jnp.zeros_like(taper))
        for slot, shifts, masks, offset in layout[half]:
            block = refs[slot]
            height = block.shape[4]
            for first, shift in enumerate(shifts):
                for second, mask in enumerate(masks):
                    row = 0
                    if paired:
                        row = pl.multiple_of(((chan ^ mask) * bls + (bl ^ shift)) * height, height)
                    for part in range(2):
                        values = block[first, second, channel + offset, part].astype(jnp.float32)
                        column = (2 * (1 - which) + part) * HALF
                        stack_ref[window, pl.ds(row, height), column : column + HALF] = (values * taper).astype(jnp.bfloat16)

    def store(index, window, gram):
        out_ref[index, 0, window] = (gram * scale).astype(jnp.bfloat16)

    def both(now_ref, next_ref):
        following = jnp.minimum(step + 1, channels - 1)
        waiting = None
        for window in range(halves - 1):
            straight = now_ref[window]
            late_a, late_b, early_a, early_b = (straight[:, i * HALF : (i + 1) * HALF] for i in range(4))
            crossed = jnp.concatenate([late_b, -late_a, early_b, -early_a], axis=1)
            for index, left in enumerate((straight, crossed)):
                gram = lax.dot_general(left, straight, (((1,), (1,)), ((), ())), preferred_element_type=jnp.float32)
                if waiting is not None:
                    store(*waiting)
                half, which = (window + 1, 1) if index == 0 else (window, 0)
                place(next_ref, following, window, half, which)
                waiting = (index, window, gram)
        store(*waiting)

    @pl.when(step == 0)
    def _():
        for window in range(halves - 1):
            place(even_ref, step, window, window + 1, 1)
            place(even_ref, step, window, window, 0)

    @pl.when(step % 2 == 0)
    def _():
        both(even_ref, odd_ref)

    @pl.when(step % 2 == 1)
    def _():
        both(odd_ref, even_ref)


def correlated(blocks, total, base, paired, before):
    channels = min(array.shape[2] for half in blocks for array, _, _ in half)
    parts, height, samples = blocks[0][0][0].shape[3:]
    windows = len(blocks) - 1
    everyone = sum(len(shifts) * len(masks) for _, shifts, masks in blocks[0]) * height
    flops = channels * windows * 2 * parts * everyone * everyone * 2 * parts * samples
    layout, flat = [], []
    for half in blocks:
        layout.append([])
        for array, shifts, masks in half:
            layout[-1].append((len(flat), shifts, masks, base if array.shape[2] > channels else 0))
            flat.append(array)
    given = [] if before is None else [before]

    def body(taper_ref, *refs):
        correlate(taper_ref, *refs[len(given) :], layout=layout, channels=channels, paired=paired)

    return pl.pallas_call(
        body,
        grid=(channels,),
        in_specs=[pl.BlockSpec(memory_space=pltpu.VMEM)]
        + [pl.BlockSpec(memory_space=pl.ANY)] * len(given)
        + [pl.BlockSpec(memory_space=pltpu.VMEM)] * len(flat),
        out_specs=pl.BlockSpec((parts, 1, windows, everyone, everyone), lambda c: (0, c + base, 0, 0, 0)),
        out_shape=jax.ShapeDtypeStruct((parts, total, windows, everyone, everyone), jnp.bfloat16),
        input_output_aliases={1: 0} if given else {},
        scratch_shapes=[pltpu.VMEM((windows, everyone, 2 * parts * samples), jnp.bfloat16)] * 2,
        cost_estimate=pl.CostEstimate(flops=flops, bytes_accessed=4 << 20, transcendentals=0),
        compiler_params=pltpu.CompilerParams(vmem_limit_bytes=12 << 20),
    )(tapers(samples), *given, *flat)


def picked(held, axis, cuts):
    size, block, kind = held[0].shape[0], held[0].shape[1:], held[0].dtype

    def body(*refs):
        mine, outs = lax.axis_index(axis), iter(refs[len(held) :])
        for mask in range(size):
            for start, stop in cuts[mask]:
                out_ref = next(outs)
                for place in range(len(held)):
                    out_ref[place] = refs[place][mine ^ mask, start:stop]

    shapes = [(len(held), stop - start) + block[1:] for mask in range(size) for start, stop in cuts[mask]]
    outs = pl.pallas_call(
        body,
        in_specs=[pl.BlockSpec(memory_space=pltpu.VMEM)] * len(held),
        out_specs=[pl.BlockSpec(memory_space=pltpu.VMEM)] * len(shapes),
        out_shape=[jax.ShapeDtypeStruct(shape, kind) for shape in shapes],
        compiler_params=pltpu.CompilerParams(vmem_limit_bytes=4 << 20),
        cost_estimate=pl.CostEstimate(flops=0, bytes_accessed=1 << 20, transcendentals=0),
    )(*held)
    outs = iter(outs)
    return [[next(outs) for _ in cuts[mask]] for mask in range(size)]


def staged(voltages):
    parts, signals, channels, samples = voltages.shape
    chans, bls = lax.axis_size("chan"), lax.axis_size("bl")
    each = channels // (chans * bls)
    halves = samples // HALF
    masks, shifts = range(chans), range(bls)
    order = shifts[1:]
    split = voltages.reshape(parts, signals, chans, bls, each, samples)

    def cut(half):
        def body(whole_ref, *rest):
            outs, sems = rest[:-1], rest[-1]
            axis, count = ("bl", bls) if half == halves - 1 else ("chan", chans)
            mine, copies = lax.axis_index(axis), []
            for mask in range(count):
                place = (slice(None), slice(None), pl.ds(mine ^ mask, 1))
                if axis == "bl":
                    place = (slice(None), slice(None), slice(None), pl.ds(mine ^ mask, 1))
                source = whole_ref.at[place + (Ellipsis, pl.ds(half * HALF, HALF))]
                copies.append(pltpu.make_async_copy(source, outs[mask], sems.at[mask]))
            for copy in copies:
                copy.start()
            for copy in copies:
                copy.wait()

        bl_part = half == halves - 1
        shape = (parts, signals, chans if bl_part else 1, 1 if bl_part else bls, each, HALF)
        count = bls if bl_part else chans
        return pl.pallas_call(
            body,
            in_specs=[pl.BlockSpec(memory_space=pl.ANY)],
            out_specs=[pl.BlockSpec(memory_space=pltpu.VMEM)] * count,
            out_shape=[jax.ShapeDtypeStruct(shape, voltages.dtype)] * count,
            scratch_shapes=[pltpu.SemaphoreType.DMA((count,))],
            compiler_params=pltpu.CompilerParams(vmem_limit_bytes=4 << 20),
            cost_estimate=pl.CostEstimate(flops=0, bytes_accessed=2 << 20, transcendentals=0),
        )(split)

    def sliced(pieces, mask):
        part = pieces[mask].reshape(parts, signals, -1, each, HALF)
        return jnp.transpose(part, (2, 3, 0, 1, 4))

    whole = [(0, each)]
    bounds = sorted({0, each * 3 // 8, each * 6 // 8, each})
    split_cuts = list(zip(bounds, bounds[1:]))

    def over_chan_first(half):
        pieces = cut(half)
        held = [sliced(pieces, 0)]
        for mask in masks[1:]:
            held.append(exchanged(sliced(pieces, mask), "chan", mask))
        outgoing = picked(held, "bl", [whole] + [split_cuts] * (bls - 1))
        result = [[(outgoing[0][0][None], [0], masks)] for _ in split_cuts]
        for part in range(len(split_cuts)):
            for shift in order:
                moved = exchanged(outgoing[shift][part], "bl", shift)
                result[part].append((moved[None], [shift], masks))
        return result

    def over_bl_first(half):
        pieces = cut(half)
        held = {0: sliced(pieces, 0)}
        for shift in order:
            held[shift] = exchanged(sliced(pieces, shift), "bl", shift)
        groups = [list(shifts[: bls // 2]), list(shifts[bls // 2 :])] if bls > 1 else [[0]]
        here, along = [], [[] for _ in split_cuts]
        for group in groups:
            outgoing = picked([held[s] for s in group], "chan", [whole] * chans)
            turned = [outgoing[0][0]]
            for mask in masks[1:]:
                turned.append(exchanged(outgoing[mask][0], "chan", mask))
            here += [(turned[mask][:, None], group, [mask]) for mask in masks]
            cuts = split_cuts if group is groups[-1] else whole
            for part, (start, stop) in enumerate(cuts):
                stacked = jnp.stack([array[:, start:stop] for array in turned], 1)
                passed = passed_along(stacked, "tm", 1)
                for target in along if len(cuts) == 1 else along[part : part + 1]:
                    target.append((passed, group, masks))
        return here, along

    last, received = over_bl_first(halves - 1)
    others = [over_chan_first(h) for h in range(halves - 1)]
    result = None
    for part, (start, stop) in enumerate(split_cuts):
        blocks = [received[part]] + [other[part] for other in others] + [last]
        result = correlated(blocks, each, start, True, result)
    return result


def turned(piece):
    parts, signals, channels, samples = piece.shape
    devices = lax.axis_size("chan") * lax.axis_size("bl")
    by_channel = jnp.transpose(piece, (2, 0, 1, 3))
    swapped = lax.all_to_all(by_channel, ("chan", "bl"), split_axis=0, concat_axis=0, tiled=True)
    swapped = swapped.reshape(devices, channels // devices, parts, signals, samples)
    swapped = jnp.transpose(swapped, (1, 2, 0, 3, 4))
    return swapped.reshape(1, 1, channels // devices, parts, devices * signals, samples)


def direct(voltages):
    halves = voltages.shape[3] // HALF
    pieces = [voltages[:, :, :, i * HALF : (i + 1) * HALF] for i in range(halves)]
    last = turned(pieces[-1])
    received = passed_along(last, "tm", 1)
    blocks = [received] + [turned(piece) for piece in pieces[:-1]] + [last]
    return correlated([[(block, [0], [0])] for block in blocks], last.shape[2], 0, False, None)


def placed(voltages):
    chans, bls = lax.axis_size("chan"), lax.axis_size("bl")
    if voltages.shape[1] % ROWS == 0 and chans <= 4 and not (chans & (chans - 1) or bls & (bls - 1)):
        return staged(voltages)
    return direct(voltages)


def solution(mesh):
    return jax.shard_map(
        placed,
        mesh=mesh,
        in_specs=(P(None, ("chan", "bl"), None, "tm"),),
        out_specs=P(None, ("chan", "bl"), "tm", None, None),
        check_vma=False,
    )
```
